32 devices in a mesh: blk: 8 (over y, x, core), frq: 4 (over z).
Axes of the slice: x: 2, y: 2, z: 4, core: 2. Of those that a mesh axis runs over, the one named last changes fastest.
Arguments:
- spectra: bfloat16 [2, 1024, 64, 512], P(None, 'blk', None, 'frq'), may hold values from -6 to 6
- live: int32 [1024], P('blk'), may hold values 0 or 1
Outputs:
- xcorr: float32 [3, 1024, 128, 128], P(None, ('blk', 'frq'))
The draws below stay inside these ranges and needn't reach their ends.
All inputs are finite; a program needn't handle non-finite values. No bound on the sum of `live` on one device may be relied on, other than what follows from the above.
Results may differ from the reference program's by a relative error of at most 0.0058.
Values may be sent and summed in bfloat16 or wider, within the bound.
No kernel may reach another device: no remote copies, remote signals or barrier semaphores. Data moves between devices by JAX's collectives and lax.ppermute only.
A program may use at most 128 MiB of HBM per device.

```python
import math
import jax
import jax.numpy as jnp
from jax import lax

BLOCK = 128
F = 512
W = 64
LAGS = 128
ROUNDS = 3
NCH = 1024
N_BLK = 8


def with_ends(result, own_key, least, largest):
    shape = result.shape
    spot = [jax.random.randint(jax.random.fold_in(own_key, axis), (), 0, shape[axis]) for axis in range(len(shape))]
    result = result.at[tuple(spot)].set(least)
    longest = shape.index(max(shape))
    spot[longest] = (spot[longest] + 1) % shape[longest]
    return result.at[tuple(spot)].set(largest)


def level_of(own_key, shape, split, least, largest):
    loudness = 1.0
    for axis_at, blocks in split:
        heights = jax.random.uniform(jax.random.fold_in(jax.random.fold_in(own_key, 6), axis_at), (blocks,), jnp.float32, least / len(split), largest / len(split))
        loudness = loudness * jnp.repeat(jnp.exp(heights), shape[axis_at] // blocks).reshape((-1,) + (1,) * (len(shape) - 1 - axis_at))
    return loudness


def scatter_about(rng, shape, deviation, bound, split=(), held_as=jnp.bfloat16):
    drawn = deviation * jax.random.normal(rng, shape, jnp.float32)
    if split:
        drawn = drawn * level_of(rng, shape, split, -0.22, 0.18)
    return jnp.clip(drawn, -bound, bound).astype(held_as)


def setup_inputs(seed: int = 0) -> dict:
    key_list = jax.random.split(jax.random.key(seed), 3)
    return {
        "spectra": scatter_about(key_list[0], (2, NCH, W, F), 1.0, 6.0, ((1, 8), (3, 4))),
        "live": with_ends((jax.random.randint(key_list[1], (NCH,), 0, 8) < 7).astype(jnp.int32), jax.random.fold_in(key_list[1], 1), 0, 1),
    }


EPSILON = 1e-06

def normalize(spectra, live):
    values = spectra.astype(jnp.float32)
    energy = lax.optimization_barrier(jnp.mean(values * values, axis=(0, 2), keepdims=True))
    weight = live.astype(jnp.float32)[None, :, None, None] * lax.rsqrt(energy + EPSILON)
    return (values * weight).astype(jnp.bfloat16)

def lag_table(first_bin, bin_count, length_all, lag_count):
    bins = first_bin + jnp.arange(bin_count, dtype=jnp.int32)
    delays = jnp.arange(lag_count, dtype=jnp.int32) - lag_count // 2
    residue = jnp.mod(bins[:, None] * delays[None, :], 2 * length_all)
    phases = residue.astype(jnp.float32) * (math.pi / length_all)
    factor = 1.0 / math.sqrt(length_all)
    return jnp.stack([jnp.cos(phases) * factor, -jnp.sin(phases) * factor], 0).astype(jnp.bfloat16)

def cross_block(local_block, remote_block):
    local_f = local_block.astype(jnp.float32)
    remote_f = remote_block.astype(jnp.float32)

    def product(left, right):
        return jnp.einsum('cwf,dwf->cdf', left, right)
    factor = 1.0 / math.sqrt(W)
    real_part = (product(local_f[0], remote_f[0]) + product(local_f[1], remote_f[1])) * factor
    imag_part = (product(local_f[1], remote_f[0]) - product(local_f[0], remote_f[1])) * factor
    return jnp.stack([real_part, imag_part], axis=2).astype(jnp.bfloat16)

def reference(spectra, live):
    normed = normalize(spectra, live)
    full_table = lag_table(0, F, F, LAGS).reshape(2 * F, LAGS)
    blocks = normed.reshape(2, N_BLK, BLOCK, W, F).transpose(1, 0, 2, 3, 4)
    results = []
    for offset in range(1, ROUNDS + 1):
        partner = jnp.roll(blocks, -offset, axis=0)

        def one_couple(couple):
            cross_spec = cross_block(couple[0], couple[1])
            lagged = jnp.dot(cross_spec.reshape(BLOCK * BLOCK, 2 * F), full_table, preferred_element_type=jnp.float32)
            return lagged.reshape(BLOCK, BLOCK, LAGS)
        lagged_all = lax.map(one_couple, (blocks, partner))
        results.append(lagged_all.reshape(NCH, BLOCK, LAGS))
    return jnp.stack(results, 0)
```

```python
import functools, math
import jax, jax.numpy as jnp
from jax import lax
from jax.experimental import pallas as pl
from jax.experimental.pallas import tpu as pltpu
from jax.sharding import PartitionSpec as P

EPSILON = 1e-06
GROUP = 16

def prep_kernel(first, live_ref, x_ref, out_ref, turned):
    parts, group, windows, bins = x_ref.shape
    taps = parts * windows
    start = (first + pl.program_id(0)) * group
    for c in range(group):
        x = x_ref[:, c].astype(jnp.float32).reshape(taps, bins)
        energy = jnp.sum(x * x, axis=0, keepdims=True) * (1.0 / taps)
        weight = live_ref[start + c].astype(jnp.float32) * lax.rsqrt(energy + EPSILON)
        turned[pl.ds(c, bins, stride=group), :] = (x * weight).T
    out_ref[...] = turned[...].reshape(bins, group, taps).astype(jnp.bfloat16)

def prepared(spectra, live, first, count):
    parts, channels, windows, bins = spectra.shape
    taps = parts * windows
    return pl.pallas_call(
        functools.partial(prep_kernel, first // GROUP),
        grid_spec=pltpu.PrefetchScalarGridSpec(
            num_scalar_prefetch=1,
            grid=(count // GROUP,),
            in_specs=[pl.BlockSpec((parts, GROUP, windows, bins), lambda g, live: (0, first // GROUP + g, 0, 0))],
            out_specs=pl.BlockSpec((bins, GROUP, taps), lambda g, live: (0, g, 0)),
            scratch_shapes=[pltpu.VMEM((bins * GROUP, taps), jnp.float32)],
        ),
        out_shape=jax.ShapeDtypeStruct((bins, count, taps), jnp.bfloat16),
        compiler_params=pltpu.CompilerParams(vmem_limit_bytes=32 << 20),
        cost_estimate=pl.CostEstimate(flops=4 * bins * count * taps * 256, bytes_accessed=4 * bins * count * taps, transcendentals=0),
        name="prep",
    )(live, spectra)

FB = 16
IB = 16

def cross_kernel(steps, pitch, *refs):
    *locals_, b_ref, table_ref, out_ref, held = refs
    fb, js, taps = b_ref.shape
    half = taps // 2
    step = pl.program_id(0)
    rows = sum(a.shape[1] for a in locals_)
    bins = steps * fb

    @pl.when(step < steps)
    def _():
        for k in range(fb):
            b = b_ref[k]
            twisted = jnp.concatenate([-b[:, half:], b[:, :half]], axis=1)
            both = jnp.concatenate([b, twisted], axis=0)
            at = 0
            for a in locals_:
                n = a.shape[1]
                c = lax.dot_general(a[k], both, (((1,), (1,)), ((), ())), preferred_element_type=jnp.float32)
                held[pl.ds(at * pitch + step * fb + k, n, stride=pitch), :] = c
                at += n

    @pl.when(step >= steps)
    def _():
        ib = out_ref.shape[0]
        first = (step - steps) * ib
        scale = 1.0 / math.sqrt(half)
        pieces = []
        for i in range(ib):
            x = held[pl.ds((first + i) * pitch, bins), :]
            xt = (x * scale).astype(jnp.bfloat16).T
            pieces.append(jnp.concatenate([xt[:js], xt[js:]], axis=1))
        lhs = jnp.concatenate(pieces, axis=0)
        y = jnp.dot(lhs, table_ref[...], preferred_element_type=jnp.float32)
        out_ref[...] = y.reshape(out_ref.shape).astype(out_ref.dtype)

def crossed(local_chunks, partner, table, fb=FB, ib=IB, pad=4):
    bins, js, taps = partner.shape
    rows = sum(a.shape[1] for a in local_chunks)
    lags = table.shape[1]
    steps = bins // fb
    pitch = bins + pad
    last = steps - 1
    return pl.pallas_call(
        functools.partial(cross_kernel, steps, pitch),
        grid=(steps + rows // ib,),
        in_specs=[pl.BlockSpec((fb, a.shape[1], taps), lambda s: (jnp.minimum(s, last), 0, 0)) for a in local_chunks]
        + [
            pl.BlockSpec((fb, js, taps), lambda s: (jnp.minimum(s, last), 0, 0)),
            pl.BlockSpec(table.shape, lambda s: (0, 0)),
        ],
        out_specs=pl.BlockSpec((ib, js, lags), lambda s: (jnp.maximum(s - steps, 0), 0, 0)),
        out_shape=jax.ShapeDtypeStruct((rows, js, lags), jnp.bfloat16),
        scratch_shapes=[pltpu.VMEM((rows * pitch, 2 * js), jnp.float32)],
        compiler_params=pltpu.CompilerParams(vmem_limit_bytes=48 << 20),
        cost_estimate=pl.CostEstimate(flops=8 * rows * js * bins * taps, bytes_accessed=2 * bins * taps * (rows + js) + 2 * rows * js * lags, transcendentals=0),
        name="cross",
    )(*local_chunks, partner, table)


F = 512
ROUNDS = 3
LAGS = 128
CHUNKS = 2


def shifted(shard, axis, by):
    length = lax.axis_size(axis)
    return lax.ppermute(shard, axis, [(i, (i + by) % length) for i in range(length)])


def lag_table(first_bin, bin_count, length_all, lag_count):
    bins = first_bin + jnp.arange(bin_count, dtype=jnp.int32)
    delays = jnp.arange(lag_count, dtype=jnp.int32) - lag_count // 2
    residue = jnp.mod(bins[:, None] * delays[None, :], 2 * length_all)
    phases = residue.astype(jnp.float32) * (math.pi / length_all)
    factor = 1.0 / math.sqrt(length_all)
    return jnp.concatenate([jnp.cos(phases) * factor, -jnp.sin(phases) * factor], 0).astype(jnp.bfloat16)


def local(spectra, live):
    channels, bins = spectra.shape[1], spectra.shape[3]
    share = channels // CHUNKS
    table = lag_table(lax.axis_index("frq") * bins, bins, F, LAGS)
    mine = [prepared(spectra, live, n * share, share) for n in range(CHUNKS)]
    partner = list(mine)
    outputs = []
    for _ in range(ROUNDS):
        pieces = []
        for n in range(CHUNKS):
            partner[n] = shifted(partner[n], "blk", -1)
            partial_sum = crossed(mine, partner[n], table)
            pieces.append(lax.psum_scatter(partial_sum, "frq", scatter_dimension=0, tiled=True))
        outputs.append(jnp.concatenate(pieces, axis=1).astype(jnp.float32))
    return jnp.stack(outputs, 0)


def solution(mesh):
    return jax.shard_map(
        local,
        mesh=mesh,
        in_specs=(P(None, "blk", None, "frq"), P("blk")),
        out_specs=P(None, ("blk", "frq"), None, None),
        check_vma=False,
    )
```
